512 devices in a mesh: vocab: 64 (over x, y, core), tok: 8 (over z).
Axes of the slice: x: 4, y: 8, z: 8, core: 2. Of those that a mesh axis runs over, the one named last changes fastest.
Arguments:
- student_hidden: bfloat16 [256, 4608], P('vocab', 'tok'), may hold values from -6 to 6
- teacher_hidden: bfloat16 [256, 4608], P('vocab', 'tok'), may hold values from -6 to 6
- student_head: bfloat16 [128000, 4608], P('vocab', 'tok'), may hold values from -0.375 to 0.375
- teacher_head: bfloat16 [128000, 4608], P('vocab', 'tok'), may hold values from -0.375 to 0.375
- token_weight: float32 [256], replicated, may hold values from 2 to 32
Outputs:
- token_kl: float32 [256], P('tok')
- hidden_grad: float32 [256, 4608], P('vocab', 'tok')
The draws below stay inside these ranges and needn't reach their ends.
All inputs are finite; a program needn't handle non-finite values.
Results may differ from the reference program's by a relative error of at most 0.0027.
Values may be sent and summed in bfloat16 or wider, within the bound.
A program may use at most 64 MiB of HBM per device.

```python
import math
import jax
import jax.numpy as jnp

D = 4608
TOKENS = 256
VOCAB = 128000


def steps_of(stream_key, shape, split, least, high):
    loudness = 1.0
    for dim, shards_of in split:
        draws = jax.random.uniform(jax.random.fold_in(jax.random.fold_in(stream_key, 6), dim), (shards_of,), jnp.float32, least / len(split), high / len(split))
        loudness = loudness * jnp.repeat(jnp.exp(draws), shape[dim] // shards_of).reshape((-1,) + (1,) * (len(shape) - 1 - dim))
    return loudness


def gaussian(own_key, extent, deviation, bound, shards=(), held_as=jnp.bfloat16):
    level = steps_of(own_key, extent, shards, -0.22, 0.18) if shards else 1.0
    values = jax.random.normal(own_key, extent, jnp.float32) * deviation * level
    return jnp.minimum(jnp.maximum(values, -bound), bound).astype(held_as)


def setup_inputs(seed: int = 0) -> dict:
    splits = jax.random.split(jax.random.key(seed), 6)
    return {
        "student_hidden": gaussian(splits[0], (TOKENS, D), 1.0, 6.0, ((0, 64), (1, 8))),
        "teacher_hidden": gaussian(splits[1], (TOKENS, D), 1.0, 6.0, ((0, 64), (1, 8))),
        "student_head": gaussian(splits[2], (VOCAB, D), (D // 16) ** -0.5, 0.375, ((0, 64), (1, 8))),
        "teacher_head": gaussian(splits[3], (VOCAB, D), (D // 16) ** -0.5, 0.375, ((0, 64), (1, 8))),
        "token_weight": jnp.clip(jnp.exp(jax.random.uniform(splits[4], (TOKENS,), jnp.float32, math.log(2.0), math.log(32.0))), 2.0, 32.0),
    }


softcap = 30.0


def reference(student_hidden, teacher_hidden, student_head, teacher_head, token_weight):
    student_raw = jnp.dot(student_hidden, student_head.T, preferred_element_type=jnp.float32)
    teacher_raw = jnp.dot(teacher_hidden, teacher_head.T, preferred_element_type=jnp.float32)
    student_logits = softcap * jnp.tanh(student_raw / softcap)
    teacher_logits = softcap * jnp.tanh(teacher_raw / softcap)
    student_exp = jnp.exp(student_logits)
    teacher_exp = jnp.exp(teacher_logits)
    student_total = jnp.sum(student_exp, axis=1)
    teacher_total = jnp.sum(teacher_exp, axis=1)
    cross = jnp.sum(teacher_exp * (teacher_logits - student_logits), axis=1)
    token_kl = cross / teacher_total - jnp.log(teacher_total) + jnp.log(student_total)
    slope = 1.0 - (student_logits / softcap) ** 2
    grad_logits = (token_weight[:, None] * (student_exp / student_total[:, None] - teacher_exp / teacher_total[:, None]) * slope).astype(jnp.bfloat16)
    hidden_grad = jnp.dot(grad_logits, student_head, preferred_element_type=jnp.float32)
    return token_kl, hidden_grad
```

```python
import functools

import jax
import jax.numpy as jnp
from jax import lax
from jax.experimental import pallas as pl
from jax.experimental.pallas import tpu as pltpu
from jax.sharding import PartitionSpec as P

MESH = pl.DeviceIdType.MESH
f32, bf16 = jnp.float32, jnp.bfloat16
softcap = 30.0

def program(
    dims, sh_ref, th_ref, w_ref, sH_ref, tH_ref, kl_ref, hg_ref,
    H, hrecv, G, S, Pt, sbuf, rbuf, As, At, acc, st_own, st_in, gbuf, hgb, ecr, es, ey, exs, ex,
    hsem, a1s, a1r, a2r, a3r, a4r, a23s, a4s, bs, br, cs, cr, ds_, dr, ecs, ecrs, eys, eyr, exs_s, exr,
):
    X, Y, Z, VR, CH, NJ = dims
    V, L, Bc = 2 * X * Y, Z // 2, X * Y // Z
    R = 8 * Bc
    T = Z * R
    v, z = lax.axis_index("vocab"), lax.axis_index("tok")
    c, chip = lax.rem(v, 2), lax.div(v, 2)
    y, x = lax.rem(chip, Y), lax.div(chip, Y)

    def at(x_, y_, c_, z_=None):
        return {"vocab": (x_ * Y + y_) * 2 + c_, "tok": z if z_ is None else z_}

    def send(src, dst, ssem, rsem, dev):
        pltpu.make_async_remote_copy(
            src_ref=src, dst_ref=dst, send_sem=ssem, recv_sem=rsem, device_id=dev, device_id_type=MESH
        ).start()

    def await_bytes(ref, sem):
        pltpu.make_async_copy(ref, ref, sem).wait()

    partner = at(x, y, 1 - c)
    beside = [at(x, y, c, lax.rem(z + 1, Z)), at(x, y, c, lax.rem(z + Z - 1, Z))]
    sign = [1, -1]

    for m, ref in enumerate((sH_ref, tH_ref)):
        pltpu.make_async_copy(ref, H.at[m, pl.ds(0, VR)], hsem.at[m]).start()

    barrier = pltpu.get_barrier_semaphore()
    greeted = [partner, *beside]
    greeted += [at(x, lax.rem(y + d, Y), c) for d in range(1, Y)]
    greeted += [at(lax.rem(x + d, X), y, c) for d in range(1, X)]
    for dev in greeted:
        pl.semaphore_signal(barrier, inc=1, device_id=dev, device_id_type=MESH)
    if NJ * CH > VR:
        for m in range(2):
            H[m, VR:, :] = jnp.zeros((NJ * CH - VR, H.shape[2]), bf16)
    pl.semaphore_wait(barrier, len(greeted))

    for m, ref in enumerate((sh_ref, th_ref)):
        send(ref, hrecv.at[m], a1s.at[m], a1r.at[m], partner)
    for m in range(2):
        await_bytes(hrecv.at[m], a1r.at[m])

    def joined(ref, m):
        own, other = ref[...].astype(f32), hrecv[m].astype(f32)
        first, second = jnp.where(c == 0, own, other), jnp.where(c == 0, other, own)
        return jnp.concatenate([first, second], axis=0)

    G[c, chip] = jnp.where(c == 0, joined(sh_ref, 0), joined(th_ref, 1)).astype(bf16)
    far_first = sorted(range(1, Y), key=lambda d: -min(d, Y - d))
    for d in far_first:
        send(G.at[c, chip], G.at[c, chip], a23s, a2r.at[d - 1], at(x, lax.rem(y + d, Y), c))

    def along_x(slot):
        for d in range(1, X):
            send(G.at[c, slot], G.at[c, slot], a23s, a3r.at[d - 1], at(lax.rem(x + d, X), y, c))

    along_x(chip)
    for d in reversed(far_first):
        slot = x * Y + lax.rem(y + Y - d, Y)
        await_bytes(G.at[c, slot], a2r.at[d - 1])
        along_x(slot)
    for d in range(X):
        row = pl.ds(lax.rem(x + X - d, X) * Y, Y)
        if d:
            await_bytes(G.at[c, row], a3r.at[d - 1])
        send(G.at[c, row], G.at[c, row], a4s, a4r.at[d], partner)
    for d in range(X):
        row = pl.ds(lax.rem(x + X - d, X) * Y, Y)
        await_bytes(G.at[1 - c, row], a4r.at[d])

    top = lax.broadcasted_iota(jnp.int32, (8, G.shape[3]), 0) < 4
    for m in range(2):

        def arrange(b, carry, m=m):
            for p in range(Bc // 2):
                a, o = G[m, b * Bc + 2 * p].astype(f32), G[m, b * Bc + 2 * p + 1].astype(f32)
                a4, o4 = pltpu.roll(a, 4, 0), pltpu.roll(o, 4, 0)
                S[m, b, p] = jnp.where(top, a, o4).astype(bf16)
                S[m, b, Bc // 2 + p] = jnp.where(top, a4, o).astype(bf16)
            return carry

        lax.fori_loop(0, Z, arrange, 0)

    for m in range(2):
        await_bytes(H.at[m, pl.ds(0, VR)], hsem.at[m])

    for k in range(L, 0, -1):

        def stage(j, carry, k=k):
            if k == L:
                for m in range(2):
                    rows = S[m].astype(f32).reshape(T, S.shape[4]).astype(bf16)
                    cols = H[m, pl.ds(pl.multiple_of(j * CH, CH), CH), :]
                    Pt[j, m] = lax.dot_general(
                        rows, cols, (((1,), (1,)), ((), ())), preferred_element_type=f32
                    )
            for m in range(2):
                for s in range(2):
                    first = L if s == m else L - 1
                    if k > first:
                        continue
                    dest = lax.rem(z + sign[s] * k + Z, Z)
                    part = Pt[j, m, pl.ds(pl.multiple_of(dest * R, R), R), :]
                    if k < first:
                        await_bytes(rbuf.at[s, k, j, m], br.at[s, k, j, m])
                        part = part + rbuf[s, k, j, m]
                    if k == L:
                        slot = j * 2 + m
                    else:
                        slot = 2 * NJ + ((L - 1 - k) * 2 + s) * 2 * NJ + j * 2 + m
                    sbuf[slot] = part
                    send(sbuf.at[slot], rbuf.at[s, k - 1, j, m], bs, br.at[s, k - 1, j, m], beside[s])
            return carry

        lax.fori_loop(0, NJ, stage, 0)

    acc[...] = jnp.zeros(acc.shape, f32)

    def finish(j, carry):
        logits = []
        for m in range(2):
            raw = Pt[j, m, pl.ds(pl.multiple_of(z * R, R), R), :]
            for s in range(2):
                await_bytes(rbuf.at[s, 0, j, m], br.at[s, 0, j, m])
                raw = raw + rbuf[s, 0, j, m]
            logits.append(jnp.tanh(raw * (1.0 / softcap)))
        held = lax.broadcasted_iota(jnp.int32, (R, CH), 1) + j * CH < VR
        slope = 1.0 - logits[0] * logits[0]
        sl, tl = softcap * logits[0], softcap * logits[1]
        se, te = jnp.where(held, jnp.exp(sl), 0.0), jnp.where(held, jnp.exp(tl), 0.0)
        As[j], At[j] = se * slope, te * slope
        for n, value in enumerate((se, te, te * (tl - sl))):
            acc[n] += functools.reduce(jnp.add, [value[:, i : i + 128] for i in range(0, CH, 128)])
        return carry

    lax.fori_loop(0, NJ, finish, 0)

    lane = lax.broadcasted_iota(jnp.int32, (R, 128), 1)
    row = lax.broadcasted_iota(jnp.int32, (R, 128), 0)
    packed = jnp.zeros((R, 128), f32)
    for n in range(3):
        packed += jnp.where(lane == row + n * R, jnp.sum(acc[n], axis=1, keepdims=True), 0.0)
    mine = jnp.sum(packed, axis=0, keepdims=True)
    st_own[...] = mine
    st_in[v] = mine

    def tell(d, carry):
        send(st_own, st_in.at[v], cs, cr, {"vocab": lax.rem(v + d, V), "tok": z})
        return carry

    lax.fori_loop(1, V, tell, 0)
    await_bytes(st_in.at[pl.ds(0, V - 1)], cr)
    total = jnp.sum(st_in[...], axis=0)
    spread = [jnp.sum(jnp.where(lane == row + n * R, total, 0.0), axis=1, keepdims=True) for n in range(3)]
    student_total, teacher_total, cross = spread

    def natural(r):
        half = R // 2
        in_core = lax.rem(r, half)
        return lax.div(in_core, 4) * 8 + lax.div(r, half) * 4 + lax.rem(in_core, 4)

    wlane = lax.broadcasted_iota(jnp.int32, (R, T), 1)
    wrow = lax.broadcasted_iota(jnp.int32, (R, T), 0)
    weight = jnp.sum(jnp.where(wlane == z * R + natural(wrow), w_ref[...], 0.0), axis=1, keepdims=True)
    student_scale, teacher_scale = weight / student_total, weight / teacher_total

    for j in range(NJ):
        gbuf[z, j] = (As[j] * student_scale - At[j] * teacher_scale).astype(bf16)
        for s in range(2):
            send(gbuf.at[z, j], gbuf.at[z, j], ds_, dr.at[s, 0, j], beside[s])

    kl = cross / teacher_total - jnp.log(teacher_total) + jnp.log(student_total)
    kl_row = jnp.sum(jnp.where(lane == natural(row), kl, 0.0), axis=0, keepdims=True)
    kl_ref[...] = kl_row[:, :R]

    half = R // 2
    blocks_in_x = Y // Bc

    def to_partner(slots, sources):
        total_ = None
        for j in range(NJ):
            rows = jnp.concatenate([gbuf[t, j] for t in sources], axis=0) if len(sources) > 1 else gbuf[sources[0], j]
            part = jnp.dot(rows, H[0, j * CH : (j + 1) * CH, :], preferred_element_type=f32)
            total_ = part if total_ is None else total_ + part
        for n, slot in enumerate(slots):
            hgb[slot] = total_[n * R : (n + 1) * R]
            theirs = pl.ds(pl.multiple_of((1 - c) * half, half), half)
            send(hgb.at[slot, theirs], ecr.at[slot], ecs, ecrs.at[slot], partner)

    def along_y(slots, sources):
        for slot, t in zip(slots, sources):
            await_bytes(ecr.at[slot], ecrs.at[slot])
            ours = pl.ds(pl.multiple_of(c * half, half), half)
            both = hgb[slot, ours] + ecr[slot]
            tx, ty = lax.div(t, blocks_in_x), lax.rem(t, blocks_in_x) * Bc
            for i in range(Bc):
                piece = both[4 * i : 4 * i + 4]
                es[slot, i] = piece

                @pl.when(ty + i == y)
                def _():
                    ey[tx * Y + y] = piece

                @pl.when(ty + i != y)
                def _():
                    send(es.at[slot, i], ey.at[tx * Y + y], eys, eyr.at[tx], at(x, ty + i, c))

    pending = ([0], [z])
    to_partner(*pending)
    for d in range(1, L + 1):
        for j in range(NJ):
            for s in range(2):
                reach = L if s == j % 2 else L - 1
                if d > reach:
                    continue
                src = lax.rem(z - sign[s] * d + Z, Z)
                await_bytes(gbuf.at[src, j], dr.at[s, d - 1, j])
                if d < reach:
                    send(gbuf.at[src, j], gbuf.at[src, j], ds_, dr.at[s, d, j], beside[s])
        if d < L:
            now = ([2 * d - 1, 2 * d], [lax.rem(z - d + Z, Z), lax.rem(z + d, Z)])
        else:
            now = ([2 * d - 1], [lax.rem(z + d, Z)])
        to_partner(*now)
        along_y(*pending)
        pending = now
    along_y(*pending)

    last = lax.div(lax.rem(z + L, Z), blocks_in_x)
    for i in range(X):
        tx = lax.rem(last + 1 + i, X)
        await_bytes(ey.at[pl.ds(0, Y - 1)], eyr.at[tx])
        summed = jnp.sum(ey[pl.ds(tx * Y, Y)], axis=0)
        exs[tx] = summed

        @pl.when(tx == x)
        def _():
            ex[x] = summed

        @pl.when(tx != x)
        def _():
            send(exs.at[tx], ex.at[x], exs_s, exr, at(tx, y, c))

    await_bytes(ex.at[pl.ds(0, X - 1)], exr)
    hg_ref[...] = jnp.sum(ex[...], axis=0)

    for m in range(2):
        await_bytes(hrecv.at[m], a1s.at[m])
    await_bytes(G.at[0, pl.ds(0, X * Y - 1)], a23s)
    await_bytes(G.at[0], a4s)
    await_bytes(sbuf, bs)
    await_bytes(st_in.at[pl.ds(0, V - 1)], cs)
    await_bytes(gbuf.at[pl.ds(0, Z - 1)], ds_)
    await_bytes(ecr, ecs)
    await_bytes(ey.at[pl.ds(0, X * (Y - 1))], eys)
    await_bytes(ex.at[pl.ds(0, X - 1)], exs_s)


def build(mesh, X, Y, Z, CH):
    V, L, Bc = 2 * X * Y, Z // 2, X * Y // Z
    R = 8 * Bc

    def per_device(student_hidden, teacher_hidden, student_head, teacher_head, token_weight):
        VR, K = student_head.shape
        NJ = -(-VR // CH)
        T = token_weight.shape[0]
        dma = pltpu.SemaphoreType.DMA
        vmem = pl.BlockSpec(memory_space=pltpu.VMEM)
        hbm = pl.BlockSpec(memory_space=pl.ANY)
        kl, hg = pl.pallas_call(
            functools.partial(program, (X, Y, Z, VR, CH, NJ)),
            out_shape=(jax.ShapeDtypeStruct((1, R), f32), jax.ShapeDtypeStruct((4, K), f32)),
            in_specs=[vmem, vmem, vmem, hbm, hbm],
            out_specs=(vmem, vmem),
            scratch_shapes=[
                pltpu.VMEM((2, NJ * CH, K), bf16),
                pltpu.VMEM((2, 4, K), bf16),
                pltpu.VMEM((2, X * Y, 8, K), bf16),
                pltpu.VMEM((2, Z, Bc, 8, K), bf16),
                pltpu.VMEM((NJ, 2, T, CH), f32),
                pltpu.VMEM((2 * NJ * (2 * L - 1), R, CH), f32),
                pltpu.VMEM((2, L, NJ, 2, R, CH), f32),
                pltpu.VMEM((NJ, R, CH), f32),
                pltpu.VMEM((NJ, R, CH), f32),
                pltpu.VMEM((3, R, 128), f32),
                pltpu.VMEM((1, 128), f32),
                pltpu.VMEM((V, 1, 128), f32),
                pltpu.VMEM((Z, NJ, R, CH), bf16),
                pltpu.VMEM((Z, R, K), f32),
                pltpu.VMEM((Z, R // 2, K), f32),
                pltpu.VMEM((Z, Bc, 4, K), f32),
                pltpu.VMEM((X * Y, 4, K), f32),
                pltpu.VMEM((X, 4, K), f32),
                pltpu.VMEM((X, 4, K), f32),
                dma((2,)),
                dma((2,)),
                dma((2,)),
                dma((Y - 1,)),
                dma((X - 1,)),
                dma((X,)),
                dma,
                dma,
                dma,
                dma((2, L, NJ, 2)),
                dma,
                dma,
                dma,
                dma((2, L, NJ)),
                dma,
                dma((Z,)),
                dma,
                dma((X,)),
                dma,
                dma,
            ],
            compiler_params=pltpu.CompilerParams(
                collective_id=0, has_side_effects=True, vmem_limit_bytes=56 * 1024 * 1024
            ),
        )(student_hidden, teacher_hidden, token_weight.reshape(1, T), student_head, teacher_head)
        return kl.reshape(R), hg

    in_specs = (P("vocab", "tok"), P("vocab", "tok"), P("vocab", "tok"), P("vocab", "tok"), P())
    return jax.shard_map(
        per_device, mesh=mesh, in_specs=in_specs, out_specs=(P("tok"), P("vocab", "tok")), check_vma=False
    )


def solution(mesh):
    return build(mesh, 4, 8, 8, 512)
```

```python
import functools

import jax
import jax.numpy as jnp
from jax import lax
from jax.experimental import pallas as pl
from jax.experimental.pallas import tpu as pltpu
from jax.sharding import PartitionSpec as P

MESH = pl.DeviceIdType.MESH
f32, bf16 = jnp.float32, jnp.bfloat16
softcap = 30.0

def program(
    dims, sh_ref, th_ref, w_ref, sH_ref, tH_ref, kl_ref, hg_ref,
    H, G, S, Pt, sbuf, rbuf, As, At, acc, st_own, st_in, gbuf, hgb, ecr, es, ey, exs, ex,
    hsem, a2r, a3r, a4r, a23s, a4s, bs, br, cs, cr, ds_, dr, ecs, ecrs, eys, eyr, exs_s, exr,
):
    X, Y, Z, VR, CH, NJ = dims
    V, L, Bc = 2 * X * Y, Z // 2, X * Y // Z
    R = 8 * Bc
    T = Z * R
    v, z = lax.axis_index("vocab"), lax.axis_index("tok")
    c, chip = lax.rem(v, 2), lax.div(v, 2)
    y, x = lax.rem(chip, Y), lax.div(chip, Y)

    def at(x_, y_, c_, z_=None):
        return {"vocab": (x_ * Y + y_) * 2 + c_, "tok": z if z_ is None else z_}

    def send(src, dst, ssem, rsem, dev):
        pltpu.make_async_remote_copy(
            src_ref=src, dst_ref=dst, send_sem=ssem, recv_sem=rsem, device_id=dev, device_id_type=MESH
        ).start()

    def await_bytes(ref, sem):
        pltpu.make_async_copy(ref, ref, sem).wait()

    partner = at(x, y, 1 - c)
    beside = [at(x, y, c, lax.rem(z + 1, Z)), at(x, y, c, lax.rem(z + Z - 1, Z))]
    sign = [1, -1]

    for m, ref in enumerate((sH_ref, tH_ref)):
        pltpu.make_async_copy(ref, H.at[m], hsem.at[m]).start()
    for m, ref in enumerate((sh_ref, th_ref)):
        G[c, chip, m] = ref[...]
    if NJ * CH > VR:
        for m in range(2):
            Pt[NJ - 1, m, :, CH - 128 :] = jnp.zeros((T, 128), f32)

    barrier = pltpu.get_barrier_semaphore()
    greeted = [partner, *beside]
    greeted += [at(x, lax.rem(y + d, Y), c) for d in range(1, Y)]
    greeted += [at(lax.rem(x + d, X), y, c) for d in range(1, X)]
    for dev in greeted:
        pl.semaphore_signal(barrier, inc=1, device_id=dev, device_id_type=MESH)
    pl.semaphore_wait(barrier, len(greeted))

    far_first = sorted(range(1, Y), key=lambda d: -min(d, Y - d))
    for d in far_first:
        send(G.at[c, chip], G.at[c, chip], a23s, a2r.at[d - 1], at(x, lax.rem(y + d, Y), c))

    def along_x(slot):
        for d in range(1, X):
            send(G.at[c, slot], G.at[c, slot], a23s, a3r.at[d - 1], at(lax.rem(x + d, X), y, c))

    along_x(chip)
    for d in reversed(far_first):
        slot = x * Y + lax.rem(y + Y - d, Y)
        await_bytes(G.at[c, slot], a2r.at[d - 1])
        along_x(slot)
    for d in range(X):
        row = pl.ds(lax.rem(x + X - d, X) * Y, Y)
        if d:
            await_bytes(G.at[c, row], a3r.at[d - 1])
        send(G.at[c, row], G.at[c, row], a4s, a4r.at[d], partner)
    for d in range(X):
        row = pl.ds(lax.rem(x + X - d, X) * Y, Y)
        await_bytes(G.at[1 - c, row], a4r.at[d])

    half = R // 2
    for m in range(2):
        for core in range(2):

            def arrange(b, carry, m=m, core=core):
                rows = [G[core, b * Bc + p, m].astype(f32) for p in range(Bc)]
                place = pl.ds(pl.multiple_of(b * R + core * half, half), half)
                S[m, place, :] = jnp.concatenate(rows, axis=0).astype(bf16)
                return carry

            lax.fori_loop(0, Z, arrange, 0)

    for m in range(2):
        await_bytes(H.at[m], hsem.at[m])

    for k in range(L, 0, -1):

        def stage(j, carry, k=k):
            if k == L:
                width = min(CH, VR - j * CH)
                for m in range(2):
                    cols = H[m, :, j * CH : j * CH + width]
                    Pt[j, m, :, :width] = jnp.dot(S[m], cols, preferred_element_type=f32)
            for m in range(2):
                for s in range(2):
                    first = L if s == m else L - 1
                    if k > first:
                        continue
                    dest = lax.rem(z + sign[s] * k + Z, Z)
                    part = Pt[j, m, pl.ds(pl.multiple_of(dest * R, R), R), :]
                    if k < first:
                        await_bytes(rbuf.at[s, k, j, m], br.at[s, k, j, m])
                        part = part + rbuf[s, k, j, m]
                    if k == L:
                        slot = j * 2 + m
                    else:
                        slot = 2 * NJ + ((L - 1 - k) * 2 + s) * 2 * NJ + j * 2 + m
                    sbuf[slot] = part
                    send(sbuf.at[slot], rbuf.at[s, k - 1, j, m], bs, br.at[s, k - 1, j, m], beside[s])
            return carry

        if k == L:
            for j in range(NJ):
                stage(j, 0)
        else:
            lax.fori_loop(0, NJ, stage, 0)

    acc[...] = jnp.zeros(acc.shape, f32)

    def finish(j, carry):
        logits = []
        for m in range(2):
            raw = Pt[j, m, pl.ds(pl.multiple_of(z * R, R), R), :]
            for s in range(2):
                await_bytes(rbuf.at[s, 0, j, m], br.at[s, 0, j, m])
                raw = raw + rbuf[s, 0, j, m]
            logits.append(jnp.tanh(raw * (1.0 / softcap)))
        held = lax.broadcasted_iota(jnp.int32, (R, CH), 1) + j * CH < VR
        slope = 1.0 - logits[0] * logits[0]
        sl, tl = softcap * logits[0], softcap * logits[1]
        se, te = jnp.where(held, jnp.exp(sl), 0.0), jnp.where(held, jnp.exp(tl), 0.0)
        As[j], At[j] = se * slope, te * slope
        for n, value in enumerate((se, te, te * (tl - sl))):
            acc[n] += functools.reduce(jnp.add, [value[:, i : i + 128] for i in range(0, CH, 128)])
        return carry

    lax.fori_loop(0, NJ, finish, 0)

    lane = lax.broadcasted_iota(jnp.int32, (R, 128), 1)
    row = lax.broadcasted_iota(jnp.int32, (R, 128), 0)
    packed = jnp.zeros((R, 128), f32)
    for n in range(3):
        packed += jnp.where(lane == row + n * R, jnp.sum(acc[n], axis=1, keepdims=True), 0.0)
    mine = jnp.sum(packed, axis=0, keepdims=True)
    st_own[...] = mine
    st_in[v] = mine

    def tell(d, carry):
        send(st_own, st_in.at[v], cs, cr, {"vocab": lax.rem(v + d, V), "tok": z})
        return carry

    lax.fori_loop(1, V, tell, 0)
    await_bytes(st_in.at[pl.ds(0, V - 1)], cr)
    total = jnp.sum(st_in[...], axis=0)
    spread = [jnp.sum(jnp.where(lane == row + n * R, total, 0.0), axis=1, keepdims=True) for n in range(3)]
    student_total, teacher_total, cross = spread

    def natural(r):
        half = R // 2
        in_core = lax.rem(r, half)
        return lax.div(in_core, 4) * 8 + lax.div(r, half) * 4 + lax.rem(in_core, 4)

    wlane = lax.broadcasted_iota(jnp.int32, (R, T), 1)
    wrow = lax.broadcasted_iota(jnp.int32, (R, T), 0)
    weight = jnp.sum(jnp.where(wlane == z * R + natural(wrow), w_ref[...], 0.0), axis=1, keepdims=True)
    student_scale, teacher_scale = weight / student_total, weight / teacher_total

    for j in range(NJ):
        gbuf[z, j] = (As[j] * student_scale - At[j] * teacher_scale).astype(bf16)
        for s in range(2):
            send(gbuf.at[z, j], gbuf.at[z, j], ds_, dr.at[s, 0, j], beside[s])

    kl = cross / teacher_total - jnp.log(teacher_total) + jnp.log(student_total)
    kl_row = jnp.sum(jnp.where(lane == natural(row), kl, 0.0), axis=0, keepdims=True)
    kl_ref[...] = kl_row[:, :R]

    blocks_in_x = Y // Bc

    def to_partner(slots, sources):
        total_ = None
        for j in range(NJ):
            width = min(CH, VR - j * CH)
            rows = jnp.concatenate([gbuf[t, j] for t in sources], axis=0) if len(sources) > 1 else gbuf[sources[0], j]
            part = lax.dot_general(
                rows[:, :width],
                H[0, :, j * CH : j * CH + width],
                (((1,), (1,)), ((), ())),
                preferred_element_type=f32,
            )
            total_ = part if total_ is None else total_ + part
        for n, slot in enumerate(slots):
            hgb[slot] = total_[n * R : (n + 1) * R]
            theirs = pl.ds(pl.multiple_of((1 - c) * half, half), half)
            send(hgb.at[slot, theirs], ecr.at[slot], ecs, ecrs.at[slot], partner)

    def along_y(slots, sources):
        for slot, t in zip(slots, sources):
            await_bytes(ecr.at[slot], ecrs.at[slot])
            ours = pl.ds(pl.multiple_of(c * half, half), half)
            both = hgb[slot, ours] + ecr[slot]
            tx, ty = lax.div(t, blocks_in_x), lax.rem(t, blocks_in_x) * Bc
            for i in range(Bc):
                piece = both[4 * i : 4 * i + 4]
                es[slot, i] = piece

                @pl.when(ty + i == y)
                def _():
                    ey[tx * Y + y] = piece

                @pl.when(ty + i != y)
                def _():
                    send(es.at[slot, i], ey.at[tx * Y + y], eys, eyr.at[tx], at(x, ty + i, c))

    pending = ([0], [z])
    to_partner(*pending)
    for d in range(1, L + 1):
        for j in range(NJ):
            for s in range(2):
                reach = L if s == j % 2 else L - 1
                if d > reach:
                    continue
                src = lax.rem(z - sign[s] * d + Z, Z)
                await_bytes(gbuf.at[src, j], dr.at[s, d - 1, j])
                if d < reach:
                    send(gbuf.at[src, j], gbuf.at[src, j], ds_, dr.at[s, d, j], beside[s])
        if d < L:
            now = ([2 * d - 1, 2 * d], [lax.rem(z - d + Z, Z), lax.rem(z + d, Z)])
        else:
            now = ([2 * d - 1], [lax.rem(z + d, Z)])
        to_partner(*now)
        along_y(*pending)
        pending = now
    along_y(*pending)

    last = lax.div(lax.rem(z + L, Z), blocks_in_x)
    for i in range(X):
        tx = lax.rem(last + 1 + i, X)
        await_bytes(ey.at[pl.ds(0, Y - 1)], eyr.at[tx])
        summed = jnp.sum(ey[pl.ds(tx * Y, Y)], axis=0)
        exs[tx] = summed

        @pl.when(tx == x)
        def _():
            ex[x] = summed

        @pl.when(tx != x)
        def _():
            send(exs.at[tx], ex.at[x], exs_s, exr, at(tx, y, c))

    await_bytes(ex.at[pl.ds(0, X - 1)], exr)
    hg_ref[...] = jnp.sum(ex[...], axis=0)

    await_bytes(G.at[0, pl.ds(0, X * Y - 1)], a23s)
    await_bytes(G.at[0], a4s)
    await_bytes(sbuf, bs)
    await_bytes(st_in.at[pl.ds(0, V - 1)], cs)
    await_bytes(gbuf.at[pl.ds(0, Z - 1)], ds_)
    await_bytes(ecr, ecs)
    await_bytes(ey.at[pl.ds(0, X * (Y - 1))], eys)
    await_bytes(ex.at[pl.ds(0, X - 1)], exs_s)


def hand_out(kl_ref, hg_ref, kl_out, hg_out):
    kl_out[...] = kl_ref[...]
    hg_out[...] = hg_ref[...]


def build(mesh, X, Y, Z, CH):
    V, L, Bc = 2 * X * Y, Z // 2, X * Y // Z
    R = 8 * Bc

    def per_device(student_hidden, teacher_hidden, student_head, teacher_head, token_weight):
        K, VR = student_head.shape[1], student_head.shape[0]
        NJ = -(-VR // CH)
        T = token_weight.shape[0]
        dma = pltpu.SemaphoreType.DMA
        vmem = pl.BlockSpec(memory_space=pltpu.VMEM)
        hbm = pl.BlockSpec(memory_space=pl.ANY)
        kl, hg = pl.pallas_call(
            functools.partial(program, (X, Y, Z, VR, CH, NJ)),
            out_shape=(jax.ShapeDtypeStruct((1, R), f32), jax.ShapeDtypeStruct((4, K), f32)),
            in_specs=[vmem, vmem, vmem, hbm, hbm],
            out_specs=(vmem, vmem),
            scratch_shapes=[
                pltpu.VMEM((2, K, VR), bf16),
                pltpu.VMEM((2, X * Y, 2, 4, K), bf16),
                pltpu.VMEM((2, T, K), bf16),
                pltpu.VMEM((NJ, 2, T, CH), f32),
                pltpu.VMEM((2 * NJ * (2 * L - 1), R, CH), f32),
                pltpu.VMEM((2, L, NJ, 2, R, CH), f32),
                pltpu.VMEM((NJ, R, CH), f32),
                pltpu.VMEM((NJ, R, CH), f32),
                pltpu.VMEM((3, R, 128), f32),
                pltpu.VMEM((1, 128), f32),
                pltpu.VMEM((V, 1, 128), f32),
                pltpu.VMEM((Z, NJ, R, CH), bf16),
                pltpu.VMEM((Z, R, K), f32),
                pltpu.VMEM((Z, R // 2, K), f32),
                pltpu.VMEM((Z, Bc, 4, K), f32),
                pltpu.VMEM((X * Y, 4, K), f32),
                pltpu.VMEM((X, 4, K), f32),
                pltpu.VMEM((X, 4, K), f32),
                dma((2,)),
                dma((Y - 1,)),
                dma((X - 1,)),
                dma((X,)),
                dma,
                dma,
                dma,
                dma((2, L, NJ, 2)),
                dma,
                dma,
                dma,
                dma((2, L, NJ)),
                dma,
                dma((Z,)),
                dma,
                dma((X,)),
                dma,
                dma,
            ],
            compiler_params=pltpu.CompilerParams(
                collective_id=0, has_side_effects=True, vmem_limit_bytes=56 * 1024 * 1024
            ),
        )(student_hidden, teacher_hidden, token_weight.reshape(1, T), student_head.T, teacher_head.T)
        kl, hg = pl.pallas_call(
            hand_out,
            out_shape=(jax.ShapeDtypeStruct((1, R), f32), jax.ShapeDtypeStruct((4, K), f32)),
            in_specs=[vmem, vmem],
            out_specs=(vmem, vmem),
        )(kl, hg)
        return kl.reshape(R), hg

    in_specs = (P("vocab", "tok"), P("vocab", "tok"), P("vocab", "tok"), P("vocab", "tok"), P())
    return jax.shard_map(
        per_device, mesh=mesh, in_specs=in_specs, out_specs=(P("tok"), P("vocab", "tok")), check_vma=False
    )


def solution(mesh):
    return build(mesh, 4, 8, 8, 512)
```

```python
import functools

import jax
import jax.numpy as jnp
from jax import lax
from jax.experimental import pallas as pl
from jax.experimental.pallas import tpu as pltpu
from jax.sharding import PartitionSpec as P

MESH = pl.DeviceIdType.MESH
f32, bf16 = jnp.float32, jnp.bfloat16
softcap = 30.0

BEND = 24.0
EDGE, ROOM = 1.01, 0.97
BASE = 251
MOST = float(BASE**3 // 2)


def power(e):
    return jnp.exp2(e).astype(bf16).astype(f32)


def encode(s):
    n = s.shape[1] // 4
    u = s / (jnp.abs(s) + BEND)
    whole = jnp.floor(u[:, 3 * n :] * MOST + 0.5)
    high = jnp.floor(whole * (1.0 / BASE**2) + 0.5)
    rest = whole - high * float(BASE**2)
    middle = jnp.floor(rest * (1.0 / BASE) + 0.5)
    low = rest - middle * float(BASE)
    fill = u[:, : 3 * n] * ROOM
    words = jnp.where(fill < 0, fill - EDGE, fill + EDGE)
    return [words[:, i * n : (i + 1) * n] * power(e) for i, e in enumerate((high, middle, low))]


def decode(words):
    n = words.shape[1] // 3
    size = jnp.abs(words)
    e = jnp.floor(jnp.log2(size))
    fill = size * power(-e) - EDGE
    a = fill / (ROOM - fill) * BEND
    first = jnp.where(words < 0, -a, a)
    u = (e[:, :n] * float(BASE**2) + e[:, n : 2 * n] * float(BASE) + e[:, 2 * n :]) * (1.0 / MOST)
    return jnp.concatenate([first, u / (1.0 - jnp.abs(u)) * BEND], axis=1)

def program(
    dims, sh_ref, th_ref, w_ref, sH_ref, tH_ref, kl_ref, hg_ref,
    H, G, S, Pt, sbuf, rbuf, As, At, acc, st_own, st_in, gbuf, hgb, ecr, es, ey, exs, ex,
    hsem, a2r, a3r, a4r, a23s, a4s, bs, br, cs, cr, ds_, dr, ecs, ecrs, eys, eyr, exs_s, exr,
):
    X, Y, Z, VR, CH, NJ = dims
    V, L, Bc = 2 * X * Y, Z // 2, X * Y // Z
    R = 8 * Bc
    T = Z * R
    v, z = lax.axis_index("vocab"), lax.axis_index("tok")
    c, chip = lax.rem(v, 2), lax.div(v, 2)
    y, x = lax.rem(chip, Y), lax.div(chip, Y)

    def at(x_, y_, c_, z_=None):
        return {"vocab": (x_ * Y + y_) * 2 + c_, "tok": z if z_ is None else z_}

    def send(src, dst, ssem, rsem, dev):
        pltpu.make_async_remote_copy(
            src_ref=src, dst_ref=dst, send_sem=ssem, recv_sem=rsem, device_id=dev, device_id_type=MESH
        ).start()

    def await_bytes(ref, sem):
        pltpu.make_async_copy(ref, ref, sem).wait()

    partner = at(x, y, 1 - c)
    beside = [at(x, y, c, lax.rem(z + 1, Z)), at(x, y, c, lax.rem(z + Z - 1, Z))]
    sign = [1, -1]

    for m, ref in enumerate((sH_ref, tH_ref)):
        pltpu.make_async_copy(ref, H.at[m], hsem.at[m]).start()
    for m, ref in enumerate((sh_ref, th_ref)):
        G[c, chip, m] = ref[...]
    if NJ * CH > VR:
        for m in range(2):
            Pt[NJ - 1, m, :, CH - 128 :] = jnp.zeros((T, 128), f32)

    barrier = pltpu.get_barrier_semaphore()
    greeted = [partner, *beside]
    greeted += [at(x, lax.rem(y + d, Y), c) for d in range(1, Y)]
    greeted += [at(lax.rem(x + d, X), y, c) for d in range(1, X)]
    for dev in greeted:
        pl.semaphore_signal(barrier, inc=1, device_id=dev, device_id_type=MESH)
    pl.semaphore_wait(barrier, len(greeted))

    far_first = sorted(range(1, Y), key=lambda d: -min(d, Y - d))
    for d in far_first:
        send(G.at[c, chip], G.at[c, chip], a23s, a2r.at[d - 1], at(x, lax.rem(y + d, Y), c))

    def along_x(slot):
        for d in range(1, X):
            send(G.at[c, slot], G.at[c, slot], a23s, a3r.at[d - 1], at(lax.rem(x + d, X), y, c))

    along_x(chip)
    for d in reversed(far_first):
        slot = x * Y + lax.rem(y + Y - d, Y)
        await_bytes(G.at[c, slot], a2r.at[d - 1])
        along_x(slot)
    for d in range(X):
        row = pl.ds(lax.rem(x + X - d, X) * Y, Y)
        if d:
            await_bytes(G.at[c, row], a3r.at[d - 1])
        send(G.at[c, row], G.at[c, row], a4s, a4r.at[d], partner)
    for d in range(X):
        row = pl.ds(lax.rem(x + X - d, X) * Y, Y)
        await_bytes(G.at[1 - c, row], a4r.at[d])

    half = R // 2
    for m in range(2):
        for core in range(2):

            def arrange(b, carry, m=m, core=core):
                rows = [G[core, b * Bc + p, m].astype(f32) for p in range(Bc)]
                place = pl.ds(pl.multiple_of(b * R + core * half, half), half)
                S[m, place, :] = jnp.concatenate(rows, axis=0).astype(bf16)
                return carry

            lax.fori_loop(0, Z, arrange, 0)

    for m in range(2):
        await_bytes(H.at[m], hsem.at[m])

    for k in range(L, 0, -1):

        def stage(j, carry, k=k):
            if k == L:
                width = min(CH, VR - j * CH)
                for m in range(2):
                    cols = H[m, :, j * CH : j * CH + width]
                    Pt[j, m, :, :width] = jnp.dot(S[m], cols, preferred_element_type=f32)
            for m in range(2):
                for s in range(2):
                    first = L if s == m else L - 1
                    if k > first:
                        continue
                    dest = lax.rem(z + sign[s] * k + Z, Z)
                    part = Pt[j, m, pl.ds(pl.multiple_of(dest * R, R), R), :]
                    if k < first:
                        await_bytes(rbuf.at[s, k, j, m], br.at[s, k, j, m])
                        part = part + decode(rbuf[s, k, j, m])
                    if k == L:
                        slot = j * 2 + m
                    else:
                        slot = 2 * NJ + ((L - 1 - k) * 2 + s) * 2 * NJ + j * 2 + m
                    for i, word in enumerate(encode(part)):
                        sbuf[slot, :, i * CH // 4 : (i + 1) * CH // 4] = word
                    send(sbuf.at[slot], rbuf.at[s, k - 1, j, m], bs, br.at[s, k - 1, j, m], beside[s])
            return carry

        if k == L:
            for j in range(NJ):
                stage(j, 0)
        else:
            lax.fori_loop(0, NJ, stage, 0)

    acc[...] = jnp.zeros(acc.shape, f32)

    def finish(j, carry):
        logits = []
        for m in range(2):
            raw = Pt[j, m, pl.ds(pl.multiple_of(z * R, R), R), :]
            for s in range(2):
                await_bytes(rbuf.at[s, 0, j, m], br.at[s, 0, j, m])
                raw = raw + decode(rbuf[s, 0, j, m])
            logits.append(jnp.tanh(raw * (1.0 / softcap)))
        held = lax.broadcasted_iota(jnp.int32, (R, CH), 1) + j * CH < VR
        slope = 1.0 - logits[0] * logits[0]
        sl, tl = softcap * logits[0], softcap * logits[1]
        se, te = jnp.where(held, jnp.exp(sl), 0.0), jnp.where(held, jnp.exp(tl), 0.0)
        As[j], At[j] = se * slope, te * slope
        for n, value in enumerate((se, te, te * (tl - sl))):
            acc[n] += functools.reduce(jnp.add, [value[:, i : i + 128] for i in range(0, CH, 128)])
        return carry

    lax.fori_loop(0, NJ, finish, 0)

    lane = lax.broadcasted_iota(jnp.int32, (R, 128), 1)
    row = lax.broadcasted_iota(jnp.int32, (R, 128), 0)
    packed = jnp.zeros((R, 128), f32)
    for n in range(3):
        packed += jnp.where(lane == row + n * R, jnp.sum(acc[n], axis=1, keepdims=True), 0.0)
    mine = jnp.sum(packed, axis=0, keepdims=True)
    st_own[...] = mine
    st_in[v] = mine

    def tell(d, carry):
        send(st_own, st_in.at[v], cs, cr, {"vocab": lax.rem(v + d, V), "tok": z})
        return carry

    lax.fori_loop(1, V, tell, 0)
    await_bytes(st_in.at[pl.ds(0, V - 1)], cr)
    total = jnp.sum(st_in[...], axis=0)
    spread = [jnp.sum(jnp.where(lane == row + n * R, total, 0.0), axis=1, keepdims=True) for n in range(3)]
    student_total, teacher_total, cross = spread

    def natural(r):
        half = R // 2
        in_core = lax.rem(r, half)
        return lax.div(in_core, 4) * 8 + lax.div(r, half) * 4 + lax.rem(in_core, 4)

    wlane = lax.broadcasted_iota(jnp.int32, (R, T), 1)
    wrow = lax.broadcasted_iota(jnp.int32, (R, T), 0)
    weight = jnp.sum(jnp.where(wlane == z * R + natural(wrow), w_ref[...], 0.0), axis=1, keepdims=True)
    student_scale, teacher_scale = weight / student_total, weight / teacher_total

    for j in range(NJ):
        gbuf[z, j] = (As[j] * student_scale - At[j] * teacher_scale).astype(bf16)
        for s in range(2):
            send(gbuf.at[z, j], gbuf.at[z, j], ds_, dr.at[s, 0, j], beside[s])

    kl = cross / teacher_total - jnp.log(teacher_total) + jnp.log(student_total)
    kl_row = jnp.sum(jnp.where(lane == natural(row), kl, 0.0), axis=0, keepdims=True)
    kl_ref[...] = kl_row[:, :R]

    blocks_in_x = Y // Bc

    def to_partner(slots, sources):
        total_ = None
        for j in range(NJ):
            width = min(CH, VR - j * CH)
            rows = jnp.concatenate([gbuf[t, j] for t in sources], axis=0) if len(sources) > 1 else gbuf[sources[0], j]
            part = lax.dot_general(
                rows[:, :width],
                H[0, :, j * CH : j * CH + width],
                (((1,), (1,)), ((), ())),
                preferred_element_type=f32,
            )
            total_ = part if total_ is None else total_ + part
        for n, slot in enumerate(slots):
            hgb[slot] = total_[n * R : (n + 1) * R]
            theirs = pl.ds(pl.multiple_of((1 - c) * half, half), half)
            send(hgb.at[slot, theirs], ecr.at[slot], ecs, ecrs.at[slot], partner)

    def along_y(slots, sources):
        for slot, t in zip(slots, sources):
            await_bytes(ecr.at[slot], ecrs.at[slot])
            ours = pl.ds(pl.multiple_of(c * half, half), half)
            both = hgb[slot, ours] + ecr[slot]
            tx, ty = lax.div(t, blocks_in_x), lax.rem(t, blocks_in_x) * Bc
            for i in range(Bc):
                piece = both[4 * i : 4 * i + 4]
                es[slot, i] = piece

                @pl.when(ty + i == y)
                def _():
                    ey[tx * Y + y] = piece

                @pl.when(ty + i != y)
                def _():
                    send(es.at[slot, i], ey.at[tx * Y + y], eys, eyr.at[tx], at(x, ty + i, c))

    pending = ([0], [z])
    to_partner(*pending)
    for d in range(1, L + 1):
        for j in range(NJ):
            for s in range(2):
                reach = L if s == j % 2 else L - 1
                if d > reach:
                    continue
                src = lax.rem(z - sign[s] * d + Z, Z)
                await_bytes(gbuf.at[src, j], dr.at[s, d - 1, j])
                if d < reach:
                    send(gbuf.at[src, j], gbuf.at[src, j], ds_, dr.at[s, d, j], beside[s])
        if d < L:
            now = ([2 * d - 1, 2 * d], [lax.rem(z - d + Z, Z), lax.rem(z + d, Z)])
        else:
            now = ([2 * d - 1], [lax.rem(z + d, Z)])
        to_partner(*now)
        along_y(*pending)
        pending = now
    along_y(*pending)

    last = lax.div(lax.rem(z + L, Z), blocks_in_x)
    for i in range(X):
        tx = lax.rem(last + 1 + i, X)
        await_bytes(ey.at[pl.ds(0, Y - 1)], eyr.at[tx])
        summed = jnp.sum(ey[pl.ds(tx * Y, Y)], axis=0)
        exs[tx] = summed

        @pl.when(tx == x)
        def _():
            ex[x] = summed

        @pl.when(tx != x)
        def _():
            send(exs.at[tx], ex.at[x], exs_s, exr, at(tx, y, c))

    await_bytes(ex.at[pl.ds(0, X - 1)], exr)
    hg_ref[...] = jnp.sum(ex[...], axis=0)

    await_bytes(G.at[0, pl.ds(0, X * Y - 1)], a23s)
    await_bytes(G.at[0], a4s)
    await_bytes(sbuf, bs)
    await_bytes(st_in.at[pl.ds(0, V - 1)], cs)
    await_bytes(gbuf.at[pl.ds(0, Z - 1)], ds_)
    await_bytes(ecr, ecs)
    await_bytes(ey.at[pl.ds(0, X * (Y - 1))], eys)
    await_bytes(ex.at[pl.ds(0, X - 1)], exs_s)


def hand_out(kl_ref, hg_ref, kl_out, hg_out):
    kl_out[...] = kl_ref[...]
    hg_out[...] = hg_ref[...]


def build(mesh, X, Y, Z, CH):
    V, L, Bc = 2 * X * Y, Z // 2, X * Y // Z
    R = 8 * Bc

    def per_device(student_hidden, teacher_hidden, student_head, teacher_head, token_weight):
        K, VR = student_head.shape[1], student_head.shape[0]
        NJ = -(-VR // CH)
        T = token_weight.shape[0]
        dma = pltpu.SemaphoreType.DMA
        vmem = pl.BlockSpec(memory_space=pltpu.VMEM)
        hbm = pl.BlockSpec(memory_space=pl.ANY)
        kl, hg = pl.pallas_call(
            functools.partial(program, (X, Y, Z, VR, CH, NJ)),
            out_shape=(jax.ShapeDtypeStruct((1, R), f32), jax.ShapeDtypeStruct((4, K), f32)),
            in_specs=[vmem, vmem, vmem, hbm, hbm],
            out_specs=(vmem, vmem),
            scratch_shapes=[
                pltpu.VMEM((2, K, VR), bf16),
                pltpu.VMEM((2, X * Y, 2, 4, K), bf16),
                pltpu.VMEM((2, T, K), bf16),
                pltpu.VMEM((NJ, 2, T, CH), f32),
                pltpu.VMEM((2 * NJ * (2 * L - 1), R, 3 * CH // 4), f32),
                pltpu.VMEM((2, L, NJ, 2, R, 3 * CH // 4), f32),
                pltpu.VMEM((NJ, R, CH), f32),
                pltpu.VMEM((NJ, R, CH), f32),
                pltpu.VMEM((3, R, 128), f32),
                pltpu.VMEM((1, 128), f32),
                pltpu.VMEM((V, 1, 128), f32),
                pltpu.VMEM((Z, NJ, R, CH), bf16),
                pltpu.VMEM((Z, R, K), f32),
                pltpu.VMEM((Z, R // 2, K), f32),
                pltpu.VMEM((Z, Bc, 4, K), f32),
                pltpu.VMEM((X * Y, 4, K), f32),
                pltpu.VMEM((X, 4, K), f32),
                pltpu.VMEM((X, 4, K), f32),
                dma((2,)),
                dma((Y - 1,)),
                dma((X - 1,)),
                dma((X,)),
                dma,
                dma,
                dma,
                dma((2, L, NJ, 2)),
                dma,
                dma,
                dma,
                dma((2, L, NJ)),
                dma,
                dma((Z,)),
                dma,
                dma((X,)),
                dma,
                dma,
            ],
            compiler_params=pltpu.CompilerParams(
                collective_id=0, has_side_effects=True, vmem_limit_bytes=56 * 1024 * 1024
            ),
        )(student_hidden, teacher_hidden, token_weight.reshape(1, T), student_head.T, teacher_head.T)
        kl, hg = pl.pallas_call(
            hand_out,
            out_shape=(jax.ShapeDtypeStruct((1, R), f32), jax.ShapeDtypeStruct((4, K), f32)),
            in_specs=[vmem, vmem],
            out_specs=(vmem, vmem),
        )(kl, hg)
        return kl.reshape(R), hg

    in_specs = (P("vocab", "tok"), P("vocab", "tok"), P("vocab", "tok"), P("vocab", "tok"), P())
    return jax.shard_map(
        per_device, mesh=mesh, in_specs=in_specs, out_specs=(P("tok"), P("vocab", "tok")), check_vma=False
    )


def solution(mesh):
    return build(mesh, 4, 8, 8, 512)
```

```python
import functools

import jax
import jax.numpy as jnp
from jax import lax
from jax.experimental import pallas as pl
from jax.experimental.pallas import tpu as pltpu
from jax.sharding import PartitionSpec as P

MESH = pl.DeviceIdType.MESH
f32, bf16 = jnp.float32, jnp.bfloat16
softcap = 30.0

BEND = 24.0
EDGE, ROOM = 1.01, 0.97
BASE = 251
MOST = float(BASE**3 // 2)


def power(e):
    return jnp.exp2(e).astype(bf16).astype(f32)


def encode(s):
    n = s.shape[1] // 4
    u = s / (jnp.abs(s) + BEND)
    whole = jnp.floor(u[:, 3 * n :] * MOST + 0.5)
    high = jnp.floor(whole * (1.0 / BASE**2) + 0.5)
    rest = whole - high * float(BASE**2)
    middle = jnp.floor(rest * (1.0 / BASE) + 0.5)
    low = rest - middle * float(BASE)
    fill = u[:, : 3 * n] * ROOM
    words = jnp.where(fill < 0, fill - EDGE, fill + EDGE)
    return [words[:, i * n : (i + 1) * n] * power(e) for i, e in enumerate((high, middle, low))]


def decode(words):
    n = words.shape[1] // 3
    size = jnp.abs(words)
    e = jnp.floor(jnp.log2(size))
    fill = size * power(-e) - EDGE
    a = fill / (ROOM - fill) * BEND
    first = jnp.where(words < 0, -a, a)
    u = (e[:, :n] * float(BASE**2) + e[:, n : 2 * n] * float(BASE) + e[:, 2 * n :]) * (1.0 / MOST)
    return jnp.concatenate([first, u / (1.0 - jnp.abs(u)) * BEND], axis=1)

def program(
    dims, sh_ref, th_ref, w_ref, sH_ref, tH_ref, kl_ref, hg_ref,
    H, G, S, Pt, sbuf, rbuf, As, At, acc, st_own, st_in, gbuf, hgb, ecr, es, ey, exs, ex,
    hsem, a2r, a3r, a4r, a23s, a4s, bs, br, cs, cr, ds_, dr, ecs, ecrs, eys, eyr, exs_s, exr,
):
    X, Y, Z, VR, CH, NJ = dims
    V, L, Bc = 2 * X * Y, Z // 2, X * Y // Z
    R = 8 * Bc
    T = Z * R
    v, z = lax.axis_index("vocab"), lax.axis_index("tok")
    c, chip = lax.rem(v, 2), lax.div(v, 2)
    y, x = lax.rem(chip, Y), lax.div(chip, Y)

    def at(x_, y_, c_, z_=None):
        return {"vocab": (x_ * Y + y_) * 2 + c_, "tok": z if z_ is None else z_}

    def send(src, dst, ssem, rsem, dev):
        pltpu.make_async_remote_copy(
            src_ref=src, dst_ref=dst, send_sem=ssem, recv_sem=rsem, device_id=dev, device_id_type=MESH
        ).start()

    def await_bytes(ref, sem):
        pltpu.make_async_copy(ref, ref, sem).wait()

    partner = at(x, y, 1 - c)
    beside = [at(x, y, c, lax.rem(z + 1, Z)), at(x, y, c, lax.rem(z + Z - 1, Z))]
    sign = [1, -1]

    for m, ref in enumerate((sH_ref, tH_ref)):
        pltpu.make_async_copy(ref, H.at[m], hsem.at[m]).start()
    for m, ref in enumerate((sh_ref, th_ref)):
        G[c, chip, m] = ref[...]
    if NJ * CH > VR:
        for m in range(2):
            Pt[NJ - 1, m, :, CH - 128 :] = jnp.zeros((T, 128), f32)

    barrier = pltpu.get_barrier_semaphore()
    greeted = [partner, *beside]
    greeted += [at(x, lax.rem(y + d, Y), c) for d in range(1, Y)]
    greeted += [at(lax.rem(x + d, X), y, c) for d in range(1, X)]
    for dev in greeted:
        pl.semaphore_signal(barrier, inc=1, device_id=dev, device_id_type=MESH)
    pl.semaphore_wait(barrier, len(greeted))

    far_first = sorted(range(1, Y), key=lambda d: -min(d, Y - d))
    for d in far_first:
        send(G.at[c, chip], G.at[c, chip], a23s, a2r.at[d - 1], at(x, lax.rem(y + d, Y), c))

    halves, half = Y // Bc, R // 2
    early = lax.rem(z + L, Z)
    early_x, early_y = lax.div(early, halves), lax.rem(early, halves) * Bc
    early_d = lax.rem(x - early_x + X, X)
    starts = [early_y] + [lax.rem(early_y + n * Bc, Y) for n in range(1, halves)]

    def group(d, h):
        return pl.ds(lax.rem(x + X - d, X) * Y + starts[h], Bc)

    def across(d, h):
        send(G.at[c, group(d, h)], G.at[c, group(d, h)], a4s, a4r.at[d, h], partner)

    def along_x(from_y):
        h = lax.rem(lax.div(from_y, Bc) - lax.div(early_y, Bc) + halves, halves)
        slot = x * Y + from_y
        for d in sorted(range(1, X), key=lambda d: -min(d, X - d)):
            send(G.at[c, slot], G.at[c, slot], a23s, a3r.at[d - 1, h], at(lax.rem(x + d, X), y, c))

    along_x(y)
    for d in reversed(far_first):
        from_y = lax.rem(y + Y - d, Y)
        await_bytes(G.at[c, x * Y + from_y], a2r.at[d - 1])
        along_x(from_y)
    for h in range(halves):
        across(0, h)

    @pl.when(early_d != 0)
    def _():
        await_bytes(G.at[c, group(early_d, 0)], a3r.at[early_d - 1, 0])
        across(early_d, 0)

    def arrange(b, carry):
        for m in range(2):
            for core in range(2):
                rows = [G[core, b * Bc + p, m].astype(f32) for p in range(Bc)]
                place = pl.ds(pl.multiple_of(b * R + core * half, half), half)
                S[m, place, :] = jnp.concatenate(rows, axis=0).astype(bf16)
        return carry

    await_bytes(G.at[1 - c, group(early_d, 0)], a4r.at[early_d, 0])
    arrange(early, 0)
    for m in range(2):
        await_bytes(H.at[m], hsem.at[m])

    def multiply(j, m, rows):
        width = min(CH, VR - j * CH)
        cols = H[m, :, j * CH : j * CH + width]
        Pt[j, m, rows, :width] = jnp.dot(S[m, rows, :], cols, preferred_element_type=f32)

    for k in range(L, 0, -1):

        def stage(j, carry, k=k):
            for m in range(2):
                if k == L:
                    multiply(j, m, pl.ds(pl.multiple_of(early * R, R), R))
                elif k == L - 1:
                    multiply(j, m, pl.ds(0, T))
                for s in range(2):
                    first = L if s == m else L - 1
                    if k > first:
                        continue
                    dest = lax.rem(z + sign[s] * k + Z, Z)
                    part = Pt[j, m, pl.ds(pl.multiple_of(dest * R, R), R), :]
                    if k < first:
                        await_bytes(rbuf.at[s, k, j, m], br.at[s, k, j, m])
                        part = part + decode(rbuf[s, k, j, m])
                    if k == L:
                        slot = j * 2 + m
                    else:
                        slot = 2 * NJ + ((L - 1 - k) * 2 + s) * 2 * NJ + j * 2 + m
                    for i, word in enumerate(encode(part)):
                        sbuf[slot, :, i * CH // 4 : (i + 1) * CH // 4] = word
                    send(sbuf.at[slot], rbuf.at[s, k - 1, j, m], bs, br.at[s, k - 1, j, m], beside[s])
            return carry

        if k == L - 1:
            for d in range(1, X):
                for h in range(halves):

                    @pl.when((early_d != d) if h == 0 else (early_d >= 0))
                    def _():
                        await_bytes(G.at[c, group(d, h)], a3r.at[d - 1, h])
                        across(d, h)

            for d in range(X):
                for h in range(halves):

                    @pl.when((early_d != d) if h == 0 else (early_d >= 0))
                    def _():
                        await_bytes(G.at[1 - c, group(d, h)], a4r.at[d, h])

            lax.fori_loop(0, Z, arrange, 0)
        if k >= L - 1:
            for j in range(NJ):
                stage(j, 0)
        else:
            lax.fori_loop(0, NJ, stage, 0)

    acc[...] = jnp.zeros(acc.shape, f32)

    def finish(j, carry):
        logits = []
        for m in range(2):
            raw = Pt[j, m, pl.ds(pl.multiple_of(z * R, R), R), :]
            for s in range(2):
                await_bytes(rbuf.at[s, 0, j, m], br.at[s, 0, j, m])
                raw = raw + decode(rbuf[s, 0, j, m])
            logits.append(jnp.tanh(raw * (1.0 / softcap)))
        held = lax.broadcasted_iota(jnp.int32, (R, CH), 1) + j * CH < VR
        slope = 1.0 - logits[0] * logits[0]
        sl, tl = softcap * logits[0], softcap * logits[1]
        se, te = jnp.where(held, jnp.exp(sl), 0.0), jnp.where(held, jnp.exp(tl), 0.0)
        As[j], At[j] = se * slope, te * slope
        for n, value in enumerate((se, te, te * (tl - sl))):
            acc[n] += functools.reduce(jnp.add, [value[:, i : i + 128] for i in range(0, CH, 128)])
        return carry

    lax.fori_loop(0, NJ, finish, 0)

    lane = lax.broadcasted_iota(jnp.int32, (R, 128), 1)
    row = lax.broadcasted_iota(jnp.int32, (R, 128), 0)
    packed = jnp.zeros((R, 128), f32)
    for n in range(3):
        packed += jnp.where(lane == row + n * R, jnp.sum(acc[n], axis=1, keepdims=True), 0.0)
    mine = jnp.sum(packed, axis=0, keepdims=True)
    st_own[...] = mine
    st_in[v] = mine

    def tell(d, carry):
        send(st_own, st_in.at[v], cs, cr, {"vocab": lax.rem(v + d, V), "tok": z})
        return carry

    lax.fori_loop(1, V, tell, 0)
    await_bytes(st_in.at[pl.ds(0, V - 1)], cr)
    total = jnp.sum(st_in[...], axis=0)
    spread = [jnp.sum(jnp.where(lane == row + n * R, total, 0.0), axis=1, keepdims=True) for n in range(3)]
    student_total, teacher_total, cross = spread

    def natural(r):
        half = R // 2
        in_core = lax.rem(r, half)
        return lax.div(in_core, 4) * 8 + lax.div(r, half) * 4 + lax.rem(in_core, 4)

    wlane = lax.broadcasted_iota(jnp.int32, (R, T), 1)
    wrow = lax.broadcasted_iota(jnp.int32, (R, T), 0)
    weight = jnp.sum(jnp.where(wlane == z * R + natural(wrow), w_ref[...], 0.0), axis=1, keepdims=True)
    student_scale, teacher_scale = weight / student_total, weight / teacher_total

    for j in range(NJ):
        gbuf[z, j] = (As[j] * student_scale - At[j] * teacher_scale).astype(bf16)
        for s in range(2):
            send(gbuf.at[z, j], gbuf.at[z, j], ds_, dr.at[s, 0, j], beside[s])

    kl = cross / teacher_total - jnp.log(teacher_total) + jnp.log(student_total)
    kl_row = jnp.sum(jnp.where(lane == natural(row), kl, 0.0), axis=0, keepdims=True)
    kl_ref[...] = kl_row[:, :R]


    def product(j, sources):
        width = min(CH, VR - j * CH)
        rows = [gbuf[t, j] for t in sources]
        rows = jnp.concatenate(rows, axis=0) if len(rows) > 1 else rows[0]
        return lax.dot_general(
            rows[:, :width],
            H[0, :, j * CH : j * CH + width],
            (((1,), (1,)), ((), ())),
            preferred_element_type=f32,
        )

    def to_partner(slots, both):
        for n, slot in enumerate(slots):
            hgb[slot] = both[n * R : (n + 1) * R]
            theirs = pl.ds(pl.multiple_of((1 - c) * half, half), half)
            send(hgb.at[slot, theirs], ecr.at[slot], ecs, ecrs.at[slot], partner)

    def along_y(slots, sources):
        for slot, t in zip(slots, sources):
            await_bytes(ecr.at[slot], ecrs.at[slot])
            ours = pl.ds(pl.multiple_of(c * half, half), half)
            both = hgb[slot, ours] + ecr[slot]
            tx, ty = lax.div(t, halves), lax.rem(t, halves) * Bc
            for i in range(Bc):
                piece = both[4 * i : 4 * i + 4]
                es[slot, i] = piece

                @pl.when(ty + i == y)
                def _():
                    ey[tx * Y + y] = piece

                @pl.when(ty + i != y)
                def _():
                    send(es.at[slot, i], ey.at[tx * Y + y], eys, eyr.at[tx], at(x, ty + i, c))

    pending = ([0], [z])
    to_partner([0], functools.reduce(jnp.add, [product(j, [z]) for j in range(NJ)]))
    for d in range(1, L + 1):
        if d < L:
            now = ([2 * d - 1, 2 * d], [lax.rem(z - d + Z, Z), lax.rem(z + d, Z)])
        else:
            now = ([2 * d - 1], [lax.rem(z + d, Z)])
        both = None
        for j in range(NJ):
            for s in range(2):
                reach = L if s == j % 2 else L - 1
                if d > reach:
                    continue
                src = lax.rem(z - sign[s] * d + Z, Z)
                await_bytes(gbuf.at[src, j], dr.at[s, d - 1, j])
                if d < reach:
                    send(gbuf.at[src, j], gbuf.at[src, j], ds_, dr.at[s, d, j], beside[s])
            if d == L:
                both = product(j, now[1]) if both is None else both + product(j, now[1])
        if d < L:
            both = functools.reduce(jnp.add, [product(j, now[1]) for j in range(NJ)])
        to_partner(now[0], both)
        along_y(*pending)
        pending = now
    along_y(*pending)

    last = lax.div(lax.rem(z + L, Z), halves)
    for i in range(X):
        tx = lax.rem(last + 1 + i, X)
        await_bytes(ey.at[pl.ds(0, Y - 1)], eyr.at[tx])
        summed = jnp.sum(ey[pl.ds(tx * Y, Y)], axis=0)
        exs[tx] = summed

        @pl.when(tx == x)
        def _():
            ex[x] = summed

        @pl.when(tx != x)
        def _():
            send(exs.at[tx], ex.at[x], exs_s, exr, at(tx, y, c))

    await_bytes(ex.at[pl.ds(0, X - 1)], exr)
    hg_ref[...] = jnp.sum(ex[...], axis=0)

    await_bytes(G.at[0, pl.ds(0, X * Y - 1)], a23s)
    await_bytes(G.at[0], a4s)
    await_bytes(sbuf, bs)
    await_bytes(st_in.at[pl.ds(0, V - 1)], cs)
    await_bytes(gbuf.at[pl.ds(0, Z - 1)], ds_)
    await_bytes(ecr, ecs)
    await_bytes(ey.at[pl.ds(0, X * (Y - 1))], eys)
    await_bytes(ex.at[pl.ds(0, X - 1)], exs_s)


def hand_out(kl_ref, hg_ref, kl_out, hg_out):
    kl_out[...] = kl_ref[...]
    hg_out[...] = hg_ref[...]


def build(mesh, X, Y, Z, CH):
    V, L, Bc = 2 * X * Y, Z // 2, X * Y // Z
    R = 8 * Bc

    def per_device(student_hidden, teacher_hidden, student_head, teacher_head, token_weight):
        K, VR = student_head.shape[1], student_head.shape[0]
        NJ = -(-VR // CH)
        T = token_weight.shape[0]
        dma = pltpu.SemaphoreType.DMA
        vmem = pl.BlockSpec(memory_space=pltpu.VMEM)
        hbm = pl.BlockSpec(memory_space=pl.ANY)
        kl, hg = pl.pallas_call(
            functools.partial(program, (X, Y, Z, VR, CH, NJ)),
            out_shape=(jax.ShapeDtypeStruct((1, R), f32), jax.ShapeDtypeStruct((4, K), f32)),
            in_specs=[vmem, vmem, vmem, hbm, hbm],
            out_specs=(vmem, vmem),
            scratch_shapes=[
                pltpu.VMEM((2, K, VR), bf16),
                pltpu.VMEM((2, X * Y, 2, 4, K), bf16),
                pltpu.VMEM((2, T, K), bf16),
                pltpu.VMEM((NJ, 2, T, CH), f32),
                pltpu.VMEM((2 * NJ * (2 * L - 1), R, 3 * CH // 4), f32),
                pltpu.VMEM((2, L, NJ, 2, R, 3 * CH // 4), f32),
                pltpu.VMEM((NJ, R, CH), f32),
                pltpu.VMEM((NJ, R, CH), f32),
                pltpu.VMEM((3, R, 128), f32),
                pltpu.VMEM((1, 128), f32),
                pltpu.VMEM((V, 1, 128), f32),
                pltpu.VMEM((Z, NJ, R, CH), bf16),
                pltpu.VMEM((Z, R, K), f32),
                pltpu.VMEM((Z, R // 2, K), f32),
                pltpu.VMEM((Z, Bc, 4, K), f32),
                pltpu.VMEM((X * Y, 4, K), f32),
                pltpu.VMEM((X, 4, K), f32),
                pltpu.VMEM((X, 4, K), f32),
                dma((2,)),
                dma((Y - 1,)),
                dma((X - 1, Y // Bc)),
                dma((X, Y // Bc)),
                dma,
                dma,
                dma,
                dma((2, L, NJ, 2)),
                dma,
                dma,
                dma,
                dma((2, L, NJ)),
                dma,
                dma((Z,)),
                dma,
                dma((X,)),
                dma,
                dma,
            ],
            compiler_params=pltpu.CompilerParams(
                collective_id=0, has_side_effects=True, vmem_limit_bytes=56 * 1024 * 1024
            ),
        )(student_hidden, teacher_hidden, token_weight.reshape(1, T), student_head.T, teacher_head.T)
        kl, hg = pl.pallas_call(
            hand_out,
            out_shape=(jax.ShapeDtypeStruct((1, R), f32), jax.ShapeDtypeStruct((4, K), f32)),
            in_specs=[vmem, vmem],
            out_specs=(vmem, vmem),
        )(kl, hg)
        return kl.reshape(R), hg

    in_specs = (P("vocab", "tok"), P("vocab", "tok"), P("vocab", "tok"), P("vocab", "tok"), P())
    return jax.shard_map(
        per_device, mesh=mesh, in_specs=in_specs, out_specs=(P("tok"), P("vocab", "tok")), check_vma=False
    )


def solution(mesh):
    return build(mesh, 4, 8, 8, 512)
```

```python
import functools

import jax
import jax.numpy as jnp
from jax import lax
from jax.experimental import pallas as pl
from jax.experimental.pallas import tpu as pltpu
from jax.sharding import PartitionSpec as P

MESH = pl.DeviceIdType.MESH
f32, bf16 = jnp.float32, jnp.bfloat16
softcap = 30.0

BEND = 24.0
EDGE, ROOM = 1.01, 0.97
BASE = 251
MOST = float(BASE**3 // 2)


def power(e):
    return jnp.exp2(e).astype(bf16).astype(f32)


def encode(s):
    n = s.shape[1] // 4
    u = s / (jnp.abs(s) + BEND)
    whole = jnp.floor(u[:, 3 * n :] * MOST + 0.5)
    high = jnp.floor(whole * (1.0 / BASE**2) + 0.5)
    rest = whole - high * float(BASE**2)
    middle = jnp.floor(rest * (1.0 / BASE) + 0.5)
    low = rest - middle * float(BASE)
    fill = u[:, : 3 * n] * ROOM
    words = jnp.where(fill < 0, fill - EDGE, fill + EDGE)
    return [words[:, i * n : (i + 1) * n] * power(e) for i, e in enumerate((high, middle, low))]


def decode(words):
    n = words.shape[1] // 3
    size = jnp.abs(words)
    e = jnp.floor(jnp.log2(size))
    fill = size * power(-e) - EDGE
    a = fill / (ROOM - fill) * BEND
    first = jnp.where(words < 0, -a, a)
    u = (e[:, :n] * float(BASE**2) + e[:, n : 2 * n] * float(BASE) + e[:, 2 * n :]) * (1.0 / MOST)
    return jnp.concatenate([first, u / (1.0 - jnp.abs(u)) * BEND], axis=1)

def program(
    dims, sh_ref, th_ref, w_ref, sH_ref, tH_ref, kl_ref, hg_ref,
    H, G, S, Pt, sbuf, rbuf, As, At, acc, st_own, st_in, gbuf, hgb, ecr, es, ey, exs, ex,
    hsem, a2r, a3r, a4r, a23s, a4s, bs, br, cs, cr, ds_, dr, ecs, ecrs, eys, eyr, exs_s, exr,
):
    X, Y, Z, VR, CH, NJ = dims
    V, L, Bc = 2 * X * Y, Z // 2, X * Y // Z
    R = 8 * Bc
    T = Z * R
    v, z = lax.axis_index("vocab"), lax.axis_index("tok")
    c, chip = lax.rem(v, 2), lax.div(v, 2)
    y, x = lax.rem(chip, Y), lax.div(chip, Y)

    def at(x_, y_, c_, z_=None):
        return {"vocab": (x_ * Y + y_) * 2 + c_, "tok": z if z_ is None else z_}

    def send(src, dst, ssem, rsem, dev):
        pltpu.make_async_remote_copy(
            src_ref=src, dst_ref=dst, send_sem=ssem, recv_sem=rsem, device_id=dev, device_id_type=MESH
        ).start()

    def await_bytes(ref, sem):
        pltpu.make_async_copy(ref, ref, sem).wait()

    partner = at(x, y, 1 - c)
    beside = [at(x, y, c, lax.rem(z + 1, Z)), at(x, y, c, lax.rem(z + Z - 1, Z))]
    sign = [1, -1]

    for m, ref in enumerate((sH_ref, tH_ref)):
        pltpu.make_async_copy(ref, H.at[m], hsem.at[m]).start()
    for m, ref in enumerate((sh_ref, th_ref)):
        G[c, chip, m] = ref[...]
    if NJ * CH > VR:
        for m in range(2):
            Pt[NJ - 1, m, :, CH - 128 :] = jnp.zeros((T, 128), f32)

    barrier = pltpu.get_barrier_semaphore()
    greeted = [partner, *beside]
    greeted += [at(x, lax.rem(y + d, Y), c) for d in range(1, Y)]
    greeted += [at(lax.rem(x + d, X), y, c) for d in range(1, X)]
    for dev in greeted:
        pl.semaphore_signal(barrier, inc=1, device_id=dev, device_id_type=MESH)
    pl.semaphore_wait(barrier, len(greeted))

    far_first = sorted(range(1, Y), key=lambda d: -min(d, Y - d))
    for d in far_first:
        send(G.at[c, chip], G.at[c, chip], a23s, a2r.at[d - 1], at(x, lax.rem(y + d, Y), c))

    halves, half = Y // Bc, R // 2
    early = lax.rem(z + L, Z)
    early_x, early_y = lax.div(early, halves), lax.rem(early, halves) * Bc
    early_d = lax.rem(x - early_x + X, X)
    starts = [early_y] + [lax.rem(early_y + n * Bc, Y) for n in range(1, halves)]

    def group(d, h):
        return pl.ds(lax.rem(x + X - d, X) * Y + starts[h], Bc)

    def across(d, h):
        send(G.at[c, group(d, h)], G.at[c, group(d, h)], a4s, a4r.at[d, h], partner)

    def along_x(from_y):
        h = lax.rem(lax.div(from_y, Bc) - lax.div(early_y, Bc) + halves, halves)
        slot = x * Y + from_y
        for d in sorted(range(1, X), key=lambda d: -min(d, X - d)):
            send(G.at[c, slot], G.at[c, slot], a23s, a3r.at[d - 1, h], at(lax.rem(x + d, X), y, c))

    along_x(y)
    for d in reversed(far_first):
        from_y = lax.rem(y + Y - d, Y)
        await_bytes(G.at[c, x * Y + from_y], a2r.at[d - 1])
        along_x(from_y)
    for h in range(halves):
        across(0, h)

    @pl.when(early_d != 0)
    def _():
        await_bytes(G.at[c, group(early_d, 0)], a3r.at[early_d - 1, 0])
        across(early_d, 0)

    def arrange(b, carry):
        for m in range(2):
            for core in range(2):
                rows = [G[core, b * Bc + p, m].astype(f32) for p in range(Bc)]
                place = pl.ds(pl.multiple_of(b * R + core * half, half), half)
                S[m, place, :] = jnp.concatenate(rows, axis=0).astype(bf16)
        return carry

    await_bytes(G.at[1 - c, group(early_d, 0)], a4r.at[early_d, 0])
    arrange(early, 0)
    for m in range(2):
        await_bytes(H.at[m], hsem.at[m])

    def multiply(j, m, rows):
        width = min(CH, VR - j * CH)
        cols = H[m, :, j * CH : j * CH + width]
        Pt[j, m, rows, :width] = jnp.dot(S[m, rows, :], cols, preferred_element_type=f32)

    for k in range(L, 0, -1):

        def stage(j, carry, k=k):
            for m in range(2):
                if k == L:
                    multiply(j, m, pl.ds(pl.multiple_of(early * R, R), R))
                elif k == L - 1:
                    multiply(j, m, pl.ds(0, T))
                for s in range(2):
                    first = L if s == m else L - 1
                    if k > first:
                        continue
                    dest = lax.rem(z + sign[s] * k + Z, Z)
                    part = Pt[j, m, pl.ds(pl.multiple_of(dest * R, R), R), :]
                    if k < first:
                        await_bytes(rbuf.at[s, k, j, m], br.at[s, k, j, m])
                        part = part + decode(rbuf[s, k, j, m])
                    if k == L:
                        slot = j * 2 + m
                    else:
                        slot = 2 * NJ + ((L - 1 - k) * 2 + s) * 2 * NJ + j * 2 + m
                    for i, word in enumerate(encode(part)):
                        sbuf[slot, :, i * CH // 4 : (i + 1) * CH // 4] = word
                    send(sbuf.at[slot], rbuf.at[s, k - 1, j, m], bs, br.at[s, k - 1, j, m], beside[s])
            return carry

        if k == L - 1:
            for d in range(X):
                for h in range(halves):

                    @pl.when((early_d != d) if h == 0 else (early_d >= 0))
                    def _():
                        await_bytes(G.at[1 - c, group(d, h)], a4r.at[d, h])
                        arrange(lax.rem(x + X - d, X) * halves + lax.div(starts[h], Bc), 0)

        if k >= L - 1:
            for j in range(NJ):
                stage(j, 0)
                if k == L and j == (NJ - 1) // 2:
                    for d in range(1, X):
                        for h in range(halves):

                            @pl.when((early_d != d) if h == 0 else (early_d >= 0))
                            def _():
                                await_bytes(G.at[c, group(d, h)], a3r.at[d - 1, h])
                                across(d, h)

        else:
            lax.fori_loop(0, NJ, stage, 0)

    acc[...] = jnp.zeros(acc.shape, f32)

    def finish(j, carry):
        logits = []
        for m in range(2):
            raw = Pt[j, m, pl.ds(pl.multiple_of(z * R, R), R), :]
            for s in range(2):
                await_bytes(rbuf.at[s, 0, j, m], br.at[s, 0, j, m])
                raw = raw + decode(rbuf[s, 0, j, m])
            logits.append(jnp.tanh(raw * (1.0 / softcap)))
        held = lax.broadcasted_iota(jnp.int32, (R, CH), 1) + j * CH < VR
        slope = 1.0 - logits[0] * logits[0]
        sl, tl = softcap * logits[0], softcap * logits[1]
        se, te = jnp.where(held, jnp.exp(sl), 0.0), jnp.where(held, jnp.exp(tl), 0.0)
        As[j], At[j] = se * slope, te * slope
        for n, value in enumerate((se, te, te * (tl - sl))):
            acc[n] += functools.reduce(jnp.add, [value[:, i : i + 128] for i in range(0, CH, 128)])
        return carry

    lax.fori_loop(0, NJ, finish, 0)

    lane = lax.broadcasted_iota(jnp.int32, (R, 128), 1)
    row = lax.broadcasted_iota(jnp.int32, (R, 128), 0)
    packed = jnp.zeros((R, 128), f32)
    for n in range(3):
        packed += jnp.where(lane == row + n * R, jnp.sum(acc[n], axis=1, keepdims=True), 0.0)
    mine = jnp.sum(packed, axis=0, keepdims=True)
    st_own[...] = mine
    st_in[v] = mine

    def tell(d, carry):
        send(st_own, st_in.at[v], cs, cr, {"vocab": lax.rem(v + d, V), "tok": z})
        return carry

    lax.fori_loop(1, V, tell, 0)
    await_bytes(st_in.at[pl.ds(0, V - 1)], cr)
    total = jnp.sum(st_in[...], axis=0)
    spread = [jnp.sum(jnp.where(lane == row + n * R, total, 0.0), axis=1, keepdims=True) for n in range(3)]
    student_total, teacher_total, cross = spread

    def natural(r):
        half = R // 2
        in_core = lax.rem(r, half)
        return lax.div(in_core, 4) * 8 + lax.div(r, half) * 4 + lax.rem(in_core, 4)

    wlane = lax.broadcasted_iota(jnp.int32, (R, T), 1)
    wrow = lax.broadcasted_iota(jnp.int32, (R, T), 0)
    weight = jnp.sum(jnp.where(wlane == z * R + natural(wrow), w_ref[...], 0.0), axis=1, keepdims=True)
    student_scale, teacher_scale = weight / student_total, weight / teacher_total

    for j in range(NJ):
        gbuf[z, j] = (As[j] * student_scale - At[j] * teacher_scale).astype(bf16)
        for s in range(2):
            send(gbuf.at[z, j], gbuf.at[z, j], ds_, dr.at[s, 0, j], beside[s])

    kl = cross / teacher_total - jnp.log(teacher_total) + jnp.log(student_total)
    kl_row = jnp.sum(jnp.where(lane == natural(row), kl, 0.0), axis=0, keepdims=True)
    kl_ref[...] = kl_row[:, :R]


    def product(j, sources):
        width = min(CH, VR - j * CH)
        rows = [gbuf[t, j] for t in sources]
        rows = jnp.concatenate(rows, axis=0) if len(rows) > 1 else rows[0]
        return lax.dot_general(
            rows[:, :width],
            H[0, :, j * CH : j * CH + width],
            (((1,), (1,)), ((), ())),
            preferred_element_type=f32,
        )

    def to_partner(slots, both):
        for n, slot in enumerate(slots):
            hgb[slot] = both[n * R : (n + 1) * R]
            theirs = pl.ds(pl.multiple_of((1 - c) * half, half), half)
            send(hgb.at[slot, theirs], ecr.at[slot], ecs, ecrs.at[slot], partner)

    def along_y(slots, sources):
        for slot, t in zip(slots, sources):
            await_bytes(ecr.at[slot], ecrs.at[slot])
            ours = pl.ds(pl.multiple_of(c * half, half), half)
            both = hgb[slot, ours] + ecr[slot]
            tx, ty = lax.div(t, halves), lax.rem(t, halves) * Bc
            for i in range(Bc):
                piece = both[4 * i : 4 * i + 4]
                es[slot, i] = piece

                @pl.when(ty + i == y)
                def _():
                    ey[tx * Y + y] = piece

                @pl.when(ty + i != y)
                def _():
                    send(es.at[slot, i], ey.at[tx * Y + y], eys, eyr.at[tx], at(x, ty + i, c))

    pending = ([0], [z])
    to_partner([0], functools.reduce(jnp.add, [product(j, [z]) for j in range(NJ)]))
    for d in range(1, L + 1):
        if d < L:
            now = ([2 * d - 1, 2 * d], [lax.rem(z - d + Z, Z), lax.rem(z + d, Z)])
        else:
            now = ([2 * d - 1], [lax.rem(z + d, Z)])
        both = None
        for j in range(NJ):
            for s in range(2):
                reach = L if s == j % 2 else L - 1
                if d > reach:
                    continue
                src = lax.rem(z - sign[s] * d + Z, Z)
                await_bytes(gbuf.at[src, j], dr.at[s, d - 1, j])
                if d < reach:
                    send(gbuf.at[src, j], gbuf.at[src, j], ds_, dr.at[s, d, j], beside[s])
            if d == L:
                both = product(j, now[1]) if both is None else both + product(j, now[1])
        if d < L:
            both = functools.reduce(jnp.add, [product(j, now[1]) for j in range(NJ)])
        to_partner(now[0], both)
        along_y(*pending)
        pending = now
    along_y(*pending)

    last = lax.div(lax.rem(z + L, Z), halves)
    for i in range(X):
        tx = lax.rem(last + 1 + i, X)
        await_bytes(ey.at[pl.ds(0, Y - 1)], eyr.at[tx])
        summed = jnp.sum(ey[pl.ds(tx * Y, Y)], axis=0)
        exs[tx] = summed

        @pl.when(tx == x)
        def _():
            ex[x] = summed

        @pl.when(tx != x)
        def _():
            send(exs.at[tx], ex.at[x], exs_s, exr, at(tx, y, c))

    await_bytes(ex.at[pl.ds(0, X - 1)], exr)
    hg_ref[...] = jnp.sum(ex[...], axis=0)

    await_bytes(G.at[0, pl.ds(0, X * Y - 1)], a23s)
    await_bytes(G.at[0], a4s)
    await_bytes(sbuf, bs)
    await_bytes(st_in.at[pl.ds(0, V - 1)], cs)
    await_bytes(gbuf.at[pl.ds(0, Z - 1)], ds_)
    await_bytes(ecr, ecs)
    await_bytes(ey.at[pl.ds(0, X * (Y - 1))], eys)
    await_bytes(ex.at[pl.ds(0, X - 1)], exs_s)


def hand_out(kl_ref, hg_ref, kl_out, hg_out):
    kl_out[...] = kl_ref[...]
    hg_out[...] = hg_ref[...]


def build(mesh, X, Y, Z, CH):
    V, L, Bc = 2 * X * Y, Z // 2, X * Y // Z
    R = 8 * Bc

    def per_device(student_hidden, teacher_hidden, student_head, teacher_head, token_weight):
        K, VR = student_head.shape[1], student_head.shape[0]
        NJ = -(-VR // CH)
        T = token_weight.shape[0]
        dma = pltpu.SemaphoreType.DMA
        vmem = pl.BlockSpec(memory_space=pltpu.VMEM)
        hbm = pl.BlockSpec(memory_space=pl.ANY)
        kl, hg = pl.pallas_call(
            functools.partial(program, (X, Y, Z, VR, CH, NJ)),
            out_shape=(jax.ShapeDtypeStruct((1, R), f32), jax.ShapeDtypeStruct((4, K), f32)),
            in_specs=[vmem, vmem, vmem, hbm, hbm],
            out_specs=(vmem, vmem),
            scratch_shapes=[
                pltpu.VMEM((2, K, VR), bf16),
                pltpu.VMEM((2, X * Y, 2, 4, K), bf16),
                pltpu.VMEM((2, T, K), bf16),
                pltpu.VMEM((NJ, 2, T, CH), f32),
                pltpu.VMEM((2 * NJ * (2 * L - 1), R, 3 * CH // 4), f32),
                pltpu.VMEM((2, L, NJ, 2, R, 3 * CH // 4), f32),
                pltpu.VMEM((NJ, R, CH), f32),
                pltpu.VMEM((NJ, R, CH), f32),
                pltpu.VMEM((3, R, 128), f32),
                pltpu.VMEM((1, 128), f32),
                pltpu.VMEM((V, 1, 128), f32),
                pltpu.VMEM((Z, NJ, R, CH), bf16),
                pltpu.VMEM((Z, R, K), f32),
                pltpu.VMEM((Z, R // 2, K), f32),
                pltpu.VMEM((Z, Bc, 4, K), f32),
                pltpu.VMEM((X * Y, 4, K), f32),
                pltpu.VMEM((X, 4, K), f32),
                pltpu.VMEM((X, 4, K), f32),
                dma((2,)),
                dma((Y - 1,)),
                dma((X - 1, Y // Bc)),
                dma((X, Y // Bc)),
                dma,
                dma,
                dma,
                dma((2, L, NJ, 2)),
                dma,
                dma,
                dma,
                dma((2, L, NJ)),
                dma,
                dma((Z,)),
                dma,
                dma((X,)),
                dma,
                dma,
            ],
            compiler_params=pltpu.CompilerParams(
                collective_id=0, has_side_effects=True, vmem_limit_bytes=56 * 1024 * 1024
            ),
        )(student_hidden, teacher_hidden, token_weight.reshape(1, T), student_head.T, teacher_head.T)
        kl, hg = pl.pallas_call(
            hand_out,
            out_shape=(jax.ShapeDtypeStruct((1, R), f32), jax.ShapeDtypeStruct((4, K), f32)),
            in_specs=[vmem, vmem],
            out_specs=(vmem, vmem),
        )(kl, hg)
        return kl.reshape(R), hg

    in_specs = (P("vocab", "tok"), P("vocab", "tok"), P("vocab", "tok"), P("vocab", "tok"), P())
    return jax.shard_map(
        per_device, mesh=mesh, in_specs=in_specs, out_specs=(P("tok"), P("vocab", "tok")), check_vma=False
    )


def solution(mesh):
    return build(mesh, 4, 8, 8, 512)
```
